32 devices in a mesh: dp: 2 (over core), seq: 4 (over y, x), tensor: 4 (over z).
Axes of the slice: x: 2, y: 2, z: 4, core: 2. Of those that a mesh axis runs over, the one named last changes fastest.
Arguments:
- tokens: bfloat16 [2, 2048, 2048], P('dp', ('seq', 'tensor')), may hold values from -6 to 6
- attn_gain: float32 [2048], replicated, may hold values from 0.5 to 1.5
- w_qkv: bfloat16 [3, 2048, 2048], P(None, None, 'tensor'), may hold values from -1 to 1
- w_out: bfloat16 [2048, 2048], P('tensor'), may hold values from -0.125 to 0.125
- mlp_gain: float32 [2048], replicated, may hold values from 0.5 to 1.5
- w_up: bfloat16 [2048, 8192], P(None, 'tensor'), may hold values from -0.125 to 0.125
- w_down: bfloat16 [8192, 2048], P('tensor'), may hold values from -0.0625 to 0.0625
- pool_gain: float32 [2048], replicated, may hold values from -8 to 8
- pool_bias: float32 [2048], replicated, may hold values from 0.5 to 5
- value_weight: float32 [2048], replicated, may hold values from -6 to 6
- valid_frames: int32 [2], replicated, may hold values from 4 to 8, as said below
Outputs:
- hidden: bfloat16 [2, 2048, 2048], P('dp', ('seq', 'tensor'))
- frame_values: float32 [2, 8], P('dp', 'seq')
- advantages: float32 [2, 8], P('dp', 'seq')
The draws below stay inside these ranges and needn't reach their ends.
Inputs may be any that keep to these rules, and one draw needn't show every extreme that they name: `valid_frames`: at least one rollout keeps all 8 frames and at least one keeps 8 // 2 of them.
All inputs are finite; a program needn't handle non-finite values.
Results may differ from the reference program's by a relative error of at most 0.017.
Values may be sent and summed in bfloat16 or wider, within the bound.
A program may use at most 256 MiB of HBM per device.

```python
import jax
import jax.numpy as jnp
from jax import lax

D = 2048
HEADS = 16
HEAD_DIM = 128
FF = 8192
TOK_FRAME = 256
FRAMES = 8
TOKENS = 2048
ROLLOUTS = 2


def draw_tokens(key, part):
    noise_key = jax.random.fold_in(key, 11)
    values = jax.random.truncated_normal(noise_key, -6.0, 6.0, (ROLLOUTS, TOKENS, D), jnp.float32)
    return values.astype(jnp.bfloat16)


def draw_w_qkv(key, part):
    base = jax.random.truncated_normal(jax.random.fold_in(key, 21), -6.0, 6.0, (3, D, D), jnp.float32) / jnp.sqrt(jnp.float32(D))
    return base.astype(jnp.bfloat16)


def draw_valid_frames(key, part):
    base = jax.random.randint(jax.random.fold_in(key, 31), (ROLLOUTS,), FRAMES // 2, FRAMES + 1, dtype=jnp.int32)
    rank = jax.random.permutation(jax.random.fold_in(key, 32), jnp.arange(ROLLOUTS, dtype=jnp.int32))
    longest = jnp.full((ROLLOUTS,), FRAMES, jnp.int32)
    shortest = jnp.full((ROLLOUTS,), FRAMES // 2, jnp.int32)
    return jnp.where(rank == 0, longest, jnp.where(rank == 1, shortest, base)).astype(jnp.int32)


def shard_levels(stream_key, shape, split, least, high):
    level = 1.0
    for dim, parts in split:
        heights = jax.random.uniform(jax.random.fold_in(jax.random.fold_in(stream_key, 6), dim), (parts,), jnp.float32, least / len(split), high / len(split))
        level = level * jnp.repeat(jnp.exp(heights), shape[dim] // parts).reshape((-1,) + (1,) * (len(shape) - 1 - dim))
    return level


def normal_values(rng, dims, scale, reach, shards=(), held_as=jnp.bfloat16):
    array = scale * jax.random.normal(rng, dims, jnp.float32)
    if shards:
        array = array * shard_levels(rng, dims, shards, -0.22, 0.18)
    return jnp.clip(array, -reach, reach).astype(held_as)


def setup_inputs(seed: int = 0) -> dict:
    key_list = jax.random.split(jax.random.key(seed), 12)
    tokens = draw_tokens(jax.random.fold_in(key_list[11], 71), 0)
    attn_gain = jnp.clip(1.0 + 0.1 * jax.random.normal(key_list[1], (D,), jnp.float32), 0.5, 1.5)
    w_qkv = draw_w_qkv(jax.random.fold_in(key_list[11], 71), 0)
    w_out = normal_values(key_list[3], (D, D), D ** -0.5, 0.125, ((0, 4),))
    mlp_gain = jnp.clip(1.0 + 0.1 * jax.random.normal(key_list[4], (D,), jnp.float32), 0.5, 1.5)
    w_up = normal_values(key_list[5], (D, FF), D ** -0.5, 0.125, ((1, 4),))
    w_down = normal_values(key_list[6], (FF, D), FF ** -0.5, 0.0625, ((0, 4),))
    pool_gain = jnp.clip(jax.random.uniform(key_list[7], (D,), jnp.float32, -8.0, 8.0), -8.0, 8.0)
    pool_bias = jnp.clip(jax.random.uniform(key_list[8], (D,), jnp.float32, 0.5, 5.0), 0.5, 5.0)
    value_weight = normal_values(key_list[9], (D,), 1.0, 6.0, (), jnp.float32)
    valid_frames = draw_valid_frames(jax.random.fold_in(key_list[11], 71), 0)
    return dict(tokens=tokens, attn_gain=attn_gain, w_qkv=w_qkv, w_out=w_out, mlp_gain=mlp_gain, w_up=w_up, w_down=w_down, pool_gain=pool_gain, pool_bias=pool_bias, value_weight=value_weight, valid_frames=valid_frames)


def rms_norm(values, gain):
    floats = values.astype(jnp.float32)
    square = lax.optimization_barrier(jnp.mean(floats * floats, axis=-1, keepdims=True))
    return (floats * lax.rsqrt(square + 1e-05) * gain).astype(jnp.bfloat16)

def reference(tokens, attn_gain, w_qkv, w_out, mlp_gain, w_up, w_down, pool_gain, pool_bias, value_weight, valid_frames):
    scale = 1.0 / HEAD_DIM ** 0.5
    frame_of = jnp.arange(TOKENS, dtype=jnp.int32) // TOK_FRAME

    def layer(args):
        rows, length = args
        normed = rms_norm(rows, attn_gain)
        qkv = jnp.einsum('nd,cde->nce', normed.astype(jnp.float32), w_qkv.astype(jnp.float32)).astype(jnp.bfloat16)
        query = qkv[:, 0].reshape(TOKENS, HEADS, HEAD_DIM).transpose(1, 0, 2)
        keys = qkv[:, 1].reshape(TOKENS, HEADS, HEAD_DIM).transpose(1, 0, 2)
        vals = qkv[:, 2].reshape(TOKENS, HEADS, HEAD_DIM).transpose(1, 0, 2)
        allowed = (frame_of[None, :] <= frame_of[:, None]) & (frame_of[None, :] < length)

        def head(trio):
            qh, kh, vh = trio
            scores = jnp.dot(qh, kh.T, preferred_element_type=jnp.float32) * scale
            scores = jnp.where(allowed, scores, -1e+30)
            peak = lax.optimization_barrier(jnp.max(scores, axis=-1, keepdims=True))
            weights = jnp.where(allowed, jnp.exp(scores - peak), 0.0)
            total = lax.optimization_barrier(jnp.sum(weights, axis=-1, keepdims=True))
            numer = jnp.dot(weights.astype(jnp.bfloat16), vh, preferred_element_type=jnp.float32)
            return numer / total
        mixed = lax.map(head, (query, keys, vals)).transpose(1, 0, 2).reshape(TOKENS, D).astype(jnp.bfloat16)
        after_attn = (rows.astype(jnp.float32) + jnp.dot(mixed, w_out, preferred_element_type=jnp.float32)).astype(jnp.bfloat16)
        normed2 = rms_norm(after_attn, mlp_gain)
        up = jax.nn.gelu(jnp.dot(normed2, w_up, preferred_element_type=jnp.float32), approximate=True).astype(jnp.bfloat16)
        return (after_attn.astype(jnp.float32) + jnp.dot(up, w_down, preferred_element_type=jnp.float32)).astype(jnp.bfloat16)
    hidden = lax.map(layer, (tokens, valid_frames))
    means = lax.optimization_barrier(jnp.mean(hidden.astype(jnp.float32).reshape(ROLLOUTS, FRAMES, TOK_FRAME, D), axis=2))
    frame_ids = jnp.arange(FRAMES, dtype=jnp.int32)
    valid = frame_ids[None, :] < valid_frames[:, None]

    def advance(state, inputs):
        mean_f, valid_f = inputs
        gate = jax.nn.sigmoid(mean_f * pool_gain + pool_bias)
        new = gate * state + (1.0 - gate) * mean_f
        state = jnp.where(valid_f[:, None], new, state)
        return (state, state)
    start = jnp.zeros((ROLLOUTS, D), jnp.float32)
    _, states = lax.scan(advance, start, (means.transpose(1, 0, 2), valid.T))
    states = states.transpose(1, 0, 2)
    frame_values = jnp.where(valid, lax.optimization_barrier(jnp.sum(states * value_weight, axis=-1)), 0.0)
    last = frame_ids[None, :] == valid_frames[:, None] - 1
    reward = lax.optimization_barrier(jnp.sum(jnp.where(last, frame_values, 0.0), axis=1))
    gap = jnp.where(valid, reward[:, None] - frame_values, 0.0)
    count = jnp.sum(valid_frames).astype(jnp.float32)
    mean = jnp.sum(gap) / count
    centered = jnp.where(valid, gap - mean, 0.0)
    variance = jnp.sum(centered * centered) / count
    advantages = jnp.where(valid, centered * lax.rsqrt(variance + 1e-05), 0.0)
    return (hidden, frame_values, advantages)
```

```python
import functools

import jax
import jax.numpy as jnp
from jax import lax
from jax.experimental import pallas as pl
from jax.experimental.pallas import tpu as pltpu
from jax.sharding import PartitionSpec as P

HEAD_DIM = 128
TOK_FRAME = 256
LANES = 128
MESH = pl.DeviceIdType.MESH
F32 = jnp.float32
BF16 = jnp.bfloat16


def rms_norm(floats, gain):
    square = jnp.mean(floats * floats, axis=-1, keepdims=True)
    return (floats * lax.rsqrt(square + 1e-05) * gain).astype(BF16)


def kernel(
    tok, attn_gain, w_qkv_h, w_out_h, mlp_gain, w_up_h, w_down_h, pool_gain, pool_bias,
    value_weight, lens,
    hidden, small,
    w_qkv, w_out, w_up, w_down, ag1, ag2, query, kv, peak, total, acc, mixed, part, rs,
    after, upbuf, fsum, means,
    wsem, ag_s, ag_r, kv_s, kv_r, rs_s, rs_r, fs_s, fs_r, mn_s, mn_r,
):
    T, S, DP = (lax.axis_size("tensor"), lax.axis_size("seq"), lax.axis_size("dp"))
    z, me, roll = (lax.axis_index("tensor"), lax.axis_index("seq"), lax.axis_index("dp"))
    rows, width = tok.shape
    block = rows * T
    heads = query.shape[-1] // HEAD_DIM
    hcols = query.shape[-1]
    ff = w_up.shape[1]
    fr_dev = block // TOK_FRAME
    scale = 1.0 / HEAD_DIM**0.5
    right, left = (lax.rem(z + 1, T), lax.rem(z + T - 1, T))
    tile = 512

    loads = [
        pltpu.make_async_copy(src, dst, wsem.at[i])
        for i, (src, dst) in enumerate(
            ((w_qkv_h, w_qkv), (w_out_h, w_out), (w_up_h, w_up), (w_down_h, w_down))
        )
    ]
    for load in loads:
        load.start()

    barrier = pltpu.get_barrier_semaphore()
    for d in range(1, T):
        pl.semaphore_signal(barrier, 1, device_id={"tensor": lax.rem(z + d, T)}, device_id_type=MESH)
    peers = []
    for a in range(DP):
        for b in range(S):
            if a or b:
                peers.append({"dp": lax.rem(roll + a, DP), "seq": lax.rem(me + b, S)})
    for peer in peers:
        pl.semaphore_signal(barrier, 1, device_id=peer, device_id_type=MESH)

    ag1[z] = rms_norm(tok[...].astype(F32), attn_gain[...])
    pl.semaphore_wait(barrier, T - 1 + len(peers))

    def zcopy(src, dst, s_sem, r_sem, to):
        return pltpu.make_async_remote_copy(
            src_ref=src, dst_ref=dst, send_sem=s_sem, recv_sem=r_sem,
            device_id={"tensor": to}, device_id_type=MESH,
        )

    def gather(buf, which, process):
        def send(s, way):
            return zcopy(
                buf.at[s], buf.at[s], ag_s.at[which, way, s], ag_r.at[which, s],
                right if way == 0 else left,
            )

        @pl.when(z < T - 1)
        def _():
            send(z, 0).start()

        @pl.when(z > 0)
        def _():
            send(z, 1).start()

        process(z)

        def step(k, carry):
            a, b = (z - k, z + k)

            @pl.when(a >= 0)
            def _():
                send(a, 0).wait_recv()

                @pl.when(z < T - 1)
                def _():
                    send(a, 0).start()

            @pl.when(b < T)
            def _():
                send(b, 1).wait_recv()

                @pl.when(z > 0)
                def _():
                    send(b, 1).start()

            @pl.when(a >= 0)
            def _():
                process(a)

            @pl.when(b < T)
            def _():
                process(b)

            return carry

        lax.fori_loop(1, T, step, 0)

        for s in range(T):

            @pl.when((s <= z) & (z < T - 1))
            def _():
                send(s, 0).wait_send()

            @pl.when((s >= z) & (z > 0))
            def _():
                send(s, 1).wait_send()

    def scatter(buf, which):
        def send(d, way):
            return zcopy(
                buf.at[way, d], buf.at[way, d], rs_s.at[which, way, d], rs_r.at[which, way, d],
                right if way == 0 else left,
            )

        def hop(d, way, first):
            @pl.when(first)
            def _():
                buf[way, d] = part[d]

            @pl.when(jnp.logical_not(first))
            def _():
                send(d, way).wait_recv()
                buf[way, d] = (buf[way, d].astype(F32) + part[d].astype(F32)).astype(BF16)

            send(d, way).start()

        for k in range(T - 1):
            d = T - 1 - k

            @pl.when(z < d)
            def _(d=d):
                hop(d, 0, z == 0)

            @pl.when(z > k)
            def _(d=k):
                hop(d, 1, z == T - 1)

        after[...] = after[...] + part[z].astype(F32)

        @pl.when(z > 0)
        def _():
            send(z, 0).wait_recv()
            after[...] = after[...] + buf[0, z].astype(F32)

        @pl.when(z < T - 1)
        def _():
            send(z, 1).wait_recv()
            after[...] = after[...] + buf[1, z].astype(F32)

        for d in range(T):

            @pl.when(z < d)
            def _(d=d):
                send(d, 0).wait_send()

            @pl.when(z > d)
            def _(d=d):
                send(d, 1).wait_send()

    def kv_send(d, s):
        return pltpu.make_async_remote_copy(
            src_ref=kv.at[me, s], dst_ref=kv.at[me, s], send_sem=kv_s.at[d, s],
            recv_sem=kv_r.at[me, s], device_id={"seq": lax.rem(me + d, S)}, device_id_type=MESH,
        )

    def project(s):
        x = ag1[s]
        kv[me, s, 0] = jnp.dot(x, w_qkv[1], preferred_element_type=F32).astype(BF16)
        kv[me, s, 1] = jnp.dot(x, w_qkv[2], preferred_element_type=F32).astype(BF16)
        for d in range(1, S):

            @pl.when(me + d < S)
            def _(d=d):
                kv_send(d, s).start()

        query[s] = jnp.dot(x, w_qkv[0], preferred_element_type=F32).astype(BF16)

    loads[0].wait()
    gather(ag1, 0, project)

    peak[...] = jnp.full_like(peak, -1e30)
    total[...] = jnp.zeros_like(total)
    acc[...] = jnp.zeros_like(acc)
    length = lens[pl.ds(roll, 1)][0, 0:1, 0:1].astype(jnp.int32)

    def attend(j):
        q_frame = me * fr_dev + lax.broadcasted_iota(jnp.int32, (block, 1), 0) // TOK_FRAME
        k_frame = j * fr_dev + lax.broadcasted_iota(jnp.int32, (1, block), 1) // TOK_FRAME
        allowed = (k_frame <= q_frame) & (k_frame < length)

        def head(h, carry):
            cols = pl.ds(pl.multiple_of(h * HEAD_DIM, HEAD_DIM), HEAD_DIM)
            q = query[:, :, cols].reshape(block, HEAD_DIM)
            k = kv[j, :, 0, :, cols].reshape(block, HEAD_DIM)
            v = kv[j, :, 1, :, cols].reshape(block, HEAD_DIM)
            scores = lax.dot_general(q, k, (((1,), (1,)), ((), ())), preferred_element_type=F32)
            scores = jnp.where(allowed, scores * scale, -1e30)
            old = peak[h]
            new = jnp.maximum(old, jnp.max(scores, axis=-1, keepdims=True))
            weights = jnp.where(allowed, jnp.exp(scores - new), 0.0)
            shrink = jnp.exp(old - new)
            peak[h] = new
            total[h] = total[h] * shrink + jnp.sum(weights, axis=-1, keepdims=True)
            acc[h] = acc[h] * shrink + jnp.dot(weights.astype(BF16), v, preferred_element_type=F32)
            return carry

        lax.fori_loop(0, heads, head, 0)

    attend(me)

    def earlier(d, carry):
        j = me - d

        @pl.when(j >= 0)
        def _():
            for s in range(T):
                pltpu.make_async_remote_copy(
                    src_ref=kv.at[j, s], dst_ref=kv.at[j, s], send_sem=kv_s.at[0, s],
                    recv_sem=kv_r.at[j, s], device_id={"seq": lax.rem(me + 1, S)},
                    device_id_type=MESH,
                ).wait_recv()
            attend(j)

        return carry

    lax.fori_loop(1, S, earlier, 0)
    for h in range(heads):
        mixed[:, h * HEAD_DIM : (h + 1) * HEAD_DIM] = (acc[h] / total[h]).astype(BF16)

    loads[1].wait()

    def out_tile(n, carry):
        cols = pl.ds(pl.multiple_of(n * tile, tile), tile)
        res = jnp.dot(mixed[...], w_out[:, cols], preferred_element_type=F32)
        part[:, :, cols] = res.astype(BF16).reshape(T, rows, tile)
        return carry

    lax.fori_loop(0, width // tile, out_tile, 0)
    after[...] = tok[...].astype(F32)
    scatter(rs, 0)
    rounded = after[...].astype(BF16).astype(F32)
    after[...] = rounded
    ag2[z] = rms_norm(rounded, mlp_gain[...])
    loads[2].wait()
    loads[3].wait()

    def feed(s):
        def up_tile(n, carry):
            cols = pl.ds(pl.multiple_of(n * tile, tile), tile)
            res = jnp.dot(ag2[s], w_up[:, cols], preferred_element_type=F32)
            upbuf[:, cols] = jax.nn.gelu(res, approximate=True).astype(BF16)
            return carry

        lax.fori_loop(0, ff // tile, up_tile, 0)

        def down_tile(n, carry):
            cols = pl.ds(pl.multiple_of(n * tile, tile), tile)
            res = jnp.dot(upbuf[...], w_down[:, cols], preferred_element_type=F32)
            part[s, :, cols] = res.astype(BF16)
            return carry

        lax.fori_loop(0, width // tile, down_tile, 0)

    gather(ag2, 1, feed)
    scatter(rs, 1)
    out = after[...].astype(BF16)
    hidden[...] = out
    sums = jnp.sum(out.astype(F32), axis=0, keepdims=True)
    chunks = width // LANES
    for c in range(chunks):
        fsum[z, c : c + 1, :] = sums[:, c * LANES : (c + 1) * LANES]

    def fs_send(d):
        return zcopy(fsum.at[z], fsum.at[z], fs_s.at[d], fs_r.at[z], lax.rem(z + d, T))

    for d in range(1, T):
        fs_send(d).start()
    for d in range(1, T):
        o = lax.rem(z + T - d, T)
        zcopy(fsum.at[o], fsum.at[o], fs_s.at[0], fs_r.at[o], right).wait_recv()
    per = T // fr_dev
    for f in range(fr_dev):
        m = fsum[f * per]
        for s in range(f * per + 1, (f + 1) * per):
            m = m + fsum[s]
        means[roll, me, f] = m / TOK_FRAME

    def mn_send(i, peer):
        return pltpu.make_async_remote_copy(
            src_ref=means.at[roll, me], dst_ref=means.at[roll, me], send_sem=mn_s.at[i],
            recv_sem=mn_r.at[roll, me], device_id=peer, device_id_type=MESH,
        )

    for i, peer in enumerate(peers):
        mn_send(i, peer).start()
    for a in range(DP):
        for b in range(S):
            if a or b:
                ra, sb = (lax.rem(roll + a, DP), lax.rem(me + b, S))
                pltpu.make_async_remote_copy(
                    src_ref=means.at[ra, sb], dst_ref=means.at[ra, sb], send_sem=mn_s.at[0],
                    recv_sem=mn_r.at[ra, sb], device_id=peers[0], device_id_type=MESH,
                ).wait_recv()

    lane = lax.broadcasted_iota(jnp.int32, (1, LANES), 1)
    values, gaps, valids = ([], [], [])
    for r in range(DP):
        span = lens[r]

        def frame(f, carry):
            state, vec = carry
            m = means[r, f // fr_dev, lax.rem(f, fr_dev)]
            gate = jax.nn.sigmoid(m * pool_gain[...] + pool_bias[...])
            new = gate * state + (1.0 - gate) * m
            state = jnp.where(span > f.astype(F32), new, state)
            dot = jnp.sum(jnp.sum(state * value_weight[...], axis=1, keepdims=True), axis=0, keepdims=True)
            return (state, jnp.where(lane == f, dot, vec))

        zero = (jnp.zeros((chunks, LANES), F32), jnp.zeros((1, LANES), F32))
        _, vec = lax.fori_loop(0, S * fr_dev, frame, zero)
        length_r = span[0:1].astype(jnp.int32)
        ok = lane < length_r
        vec = jnp.where(ok, vec, 0.0)
        reward = jnp.sum(jnp.where(lane == length_r - 1, vec, 0.0), axis=1, keepdims=True)
        values.append(vec)
        valids.append(ok)
        gaps.append(jnp.where(ok, reward - vec, 0.0))
    count = sum(lens[r][0:1, 0:1] for r in range(DP))
    mean = sum(jnp.sum(g, axis=1, keepdims=True) for g in gaps) / count
    centered = [jnp.where(ok, g - mean, 0.0) for ok, g in zip(valids, gaps)]
    variance = sum(jnp.sum(c * c, axis=1, keepdims=True) for c in centered) / count
    for r in range(DP):
        small[r : r + 1, :] = values[r]
        small[DP + r : DP + r + 1, :] = jnp.where(
            valids[r], centered[r] * lax.rsqrt(variance + 1e-05), 0.0
        )

    for d in range(1, T):
        fs_send(d).wait_send()
    for i, peer in enumerate(peers):
        mn_send(i, peer).wait_send()
    for d in range(1, S):

        @pl.when(me + d < S)
        def _(d=d):
            for s in range(T):
                kv_send(d, s).wait_send()


def local(
    tokens, attn_gain, w_qkv, w_out, mlp_gain, w_up, w_down, pool_gain, pool_bias, value_weight,
    valid_frames,
):
    T, S, DP = (lax.axis_size("tensor"), lax.axis_size("seq"), lax.axis_size("dp"))
    rows, width = tokens.shape[1:]
    block = rows * T
    fr_dev = block // TOK_FRAME
    chunks = width // LANES
    hcols = w_qkv.shape[2]
    heads = hcols // HEAD_DIM
    assert TOK_FRAME % rows == 0 and S * fr_dev <= LANES
    lens = jnp.broadcast_to(valid_frames.astype(F32)[:, None, None], (DP, chunks, LANES))
    vm = pl.BlockSpec(memory_space=pltpu.VMEM)
    hbm = pl.BlockSpec(memory_space=pl.ANY)
    dma = pltpu.SemaphoreType.DMA
    small_rows = -(-2 * DP // 8) * 8
    hidden, small = pl.pallas_call(
        kernel,
        out_shape=(
            jax.ShapeDtypeStruct((rows, width), BF16),
            jax.ShapeDtypeStruct((small_rows, LANES), F32),
        ),
        in_specs=[vm, vm, hbm, hbm, vm, hbm, hbm, vm, vm, vm, vm],
        out_specs=(vm, vm),
        scratch_shapes=[
            pltpu.VMEM(w_qkv.shape, BF16),
            pltpu.VMEM(w_out.shape, BF16),
            pltpu.VMEM(w_up.shape, BF16),
            pltpu.VMEM(w_down.shape, BF16),
            pltpu.VMEM((T, rows, width), BF16),
            pltpu.VMEM((T, rows, width), BF16),
            pltpu.VMEM((T, rows, hcols), BF16),
            pltpu.VMEM((S, T, 2, rows, hcols), BF16),
            pltpu.VMEM((heads, block, 1), F32),
            pltpu.VMEM((heads, block, 1), F32),
            pltpu.VMEM((heads, block, HEAD_DIM), F32),
            pltpu.VMEM((block, hcols), BF16),
            pltpu.VMEM((T, rows, width), BF16),
            pltpu.VMEM((2, T, rows, width), BF16),
            pltpu.VMEM((rows, width), F32),
            pltpu.VMEM((rows, w_up.shape[1]), BF16),
            pltpu.VMEM((T, chunks, LANES), F32),
            pltpu.VMEM((DP, S, fr_dev, chunks, LANES), F32),
            dma((4,)),
            dma((2, 2, T)),
            dma((2, T)),
            dma((S, T)),
            dma((S, T)),
            dma((2, 2, T)),
            dma((2, 2, T)),
            dma((T,)),
            dma((T,)),
            dma((DP * S,)),
            dma((DP, S)),
        ],
        compiler_params=pltpu.CompilerParams(
            collective_id=0, has_side_effects=True, vmem_limit_bytes=67043328
        ),
    )(
        tokens[0],
        attn_gain[None],
        w_qkv,
        w_out,
        mlp_gain[None],
        w_up,
        w_down,
        pool_gain.reshape(chunks, LANES),
        pool_bias.reshape(chunks, LANES),
        value_weight.reshape(chunks, LANES),
        lens,
    )
    roll, seq = (lax.axis_index("dp"), lax.axis_index("seq"))
    values = lax.dynamic_slice(small, (roll, seq * fr_dev), (1, fr_dev))
    advantages = lax.dynamic_slice(small, (DP + roll, seq * fr_dev), (1, fr_dev))
    return (hidden[None], values, advantages)


def solution(mesh):
    in_specs = (
        P("dp", ("seq", "tensor"), None),
        P(),
        P(None, None, "tensor"),
        P("tensor", None),
        P(),
        P(None, "tensor"),
        P("tensor", None),
        P(),
        P(),
        P(),
        P(),
    )
    out_specs = (P("dp", ("seq", "tensor"), None), P("dp", "seq"), P("dp", "seq"))
    return jax.shard_map(local, mesh=mesh, in_specs=in_specs, out_specs=out_specs, check_vma=False)
```

```python
import functools

import jax
import jax.numpy as jnp
from jax import lax
from jax.experimental import pallas as pl
from jax.experimental.pallas import tpu as pltpu
from jax.sharding import PartitionSpec as P

HEAD_DIM = 128
TOK_FRAME = 256
LANES = 128
MESH = pl.DeviceIdType.MESH
F32 = jnp.float32
BF16 = jnp.bfloat16


def rms_norm(floats, gain):
    square = jnp.mean(floats * floats, axis=-1, keepdims=True)
    return (floats * lax.rsqrt(square + 1e-05) * gain).astype(BF16)


def kernel(
    tok, attn_gain, w_qkv_h, w_out_h, mlp_gain, w_up_h, w_down_h, pool_gain, pool_bias,
    value_weight, lens,
    hidden, small,
    w_qkv, w_out, w_up, w_down, ag1, ag2, query, kv, peak, total, acc, mixed, part, rs,
    after, upbuf, fsum, means,
    wsem, ag_s, ag_r, kv_s, kv_r, rs_s, rs_r, fs_s, fs_r, mn_s, mn_r,
):
    T, S, DP = (lax.axis_size("tensor"), lax.axis_size("seq"), lax.axis_size("dp"))
    z, me, roll = (lax.axis_index("tensor"), lax.axis_index("seq"), lax.axis_index("dp"))
    rows, width = tok.shape
    block = rows * T
    heads = query.shape[-1] // HEAD_DIM
    hcols = query.shape[-1]
    ff = w_up.shape[1]
    fr_dev = block // TOK_FRAME
    scale = 1.0 / HEAD_DIM**0.5
    right, left = (lax.rem(z + 1, T), lax.rem(z + T - 1, T))
    tile = 512

    loads = [
        pltpu.make_async_copy(src, dst, wsem.at[i])
        for i, (src, dst) in enumerate(
            ((w_qkv_h, w_qkv), (w_out_h, w_out), (w_up_h, w_up), (w_down_h, w_down))
        )
    ]
    for load in loads:
        load.start()

    barrier = pltpu.get_barrier_semaphore()
    for d in range(1, T):
        pl.semaphore_signal(barrier, 1, device_id={"tensor": lax.rem(z + d, T)}, device_id_type=MESH)
    peers = []
    for a in range(DP):
        for b in range(S):
            if a or b:
                peers.append({"dp": lax.rem(roll + a, DP), "seq": lax.rem(me + b, S)})
    for peer in peers:
        pl.semaphore_signal(barrier, 1, device_id=peer, device_id_type=MESH)

    ag1[z] = rms_norm(tok[...].astype(F32), attn_gain[...])
    pl.semaphore_wait(barrier, T - 1 + len(peers))

    def zcopy(src, dst, s_sem, r_sem, to):
        return pltpu.make_async_remote_copy(
            src_ref=src, dst_ref=dst, send_sem=s_sem, recv_sem=r_sem,
            device_id={"tensor": to}, device_id_type=MESH,
        )

    def gather(buf, which, first, size, process):
        def send(s, way):
            ref = buf.at[s, pl.ds(first, size)]
            return zcopy(
                ref, ref, ag_s.at[which, way, s], ag_r.at[which, s], right if way == 0 else left
            )

        def begin():
            @pl.when(z < T - 1)
            def _():
                send(z, 0).start()

            @pl.when(z > 0)
            def _():
                send(z, 1).start()

            process(z)

        def step(k):
            a, b = (z - k, z + k)

            @pl.when(a >= 0)
            def _():
                send(a, 0).wait_recv()

                @pl.when(z < T - 1)
                def _():
                    send(a, 0).start()

            @pl.when(b < T)
            def _():
                send(b, 1).wait_recv()

                @pl.when(z > 0)
                def _():
                    send(b, 1).start()

            @pl.when(a >= 0)
            def _():
                process(a)

            @pl.when(b < T)
            def _():
                process(b)

        def drain():
            for s in range(T):

                @pl.when((s <= z) & (z < T - 1))
                def _():
                    send(s, 0).wait_send()

                @pl.when((s >= z) & (z > 0))
                def _():
                    send(s, 1).wait_send()

        return (begin, step, drain)

    def run_gather(begin, step, drain):
        begin()

        def body(k, carry):
            step(k)
            return carry

        lax.fori_loop(1, T, body, 0)
        drain()

    def scatter(buf, which, first, size):
        span = pl.ds(first, size)

        def send(d, way):
            ref = buf.at[way, d, span]
            return zcopy(
                ref, ref, rs_s.at[which, way, d], rs_r.at[which, way, d],
                right if way == 0 else left,
            )

        def move(d, way, opens):
            @pl.when(opens)
            def _():
                buf[way, d, span] = part[d, span]

            @pl.when(jnp.logical_not(opens))
            def _():
                send(d, way).wait_recv()
                buf[way, d, span] = (
                    buf[way, d, span].astype(F32) + part[d, span].astype(F32)
                ).astype(BF16)

            send(d, way).start()

        def hop(k):
            d = T - 1 - k

            @pl.when(z < d)
            def _():
                move(d, 0, z == 0)

            @pl.when(z > k)
            def _():
                move(k, 1, z == T - 1)

        def finish():
            after[span] = after[span] + part[z, span].astype(F32)

            @pl.when(z > 0)
            def _():
                send(z, 0).wait_recv()
                after[span] = after[span] + buf[0, z, span].astype(F32)

            @pl.when(z < T - 1)
            def _():
                send(z, 1).wait_recv()
                after[span] = after[span] + buf[1, z, span].astype(F32)

        def drain():
            for d in range(T):

                @pl.when(z < d)
                def _(d=d):
                    send(d, 0).wait_send()

                @pl.when(z > d)
                def _(d=d):
                    send(d, 1).wait_send()

        return (hop, finish, drain)

    def kv_send(d, s):
        return pltpu.make_async_remote_copy(
            src_ref=kv.at[me, s], dst_ref=kv.at[me, s], send_sem=kv_s.at[d, s],
            recv_sem=kv_r.at[me, s], device_id={"seq": lax.rem(me + d, S)}, device_id_type=MESH,
        )

    def project(s):
        x = ag1[s]
        kv[me, s, 0] = jnp.dot(x, w_qkv[1], preferred_element_type=F32).astype(BF16)
        kv[me, s, 1] = jnp.dot(x, w_qkv[2], preferred_element_type=F32).astype(BF16)
        for d in range(1, S):

            @pl.when(me + d < S)
            def _(d=d):
                kv_send(d, s).start()

        query[s] = jnp.dot(x, w_qkv[0], preferred_element_type=F32).astype(BF16)

    loads[0].wait()
    run_gather(*gather(ag1, 0, 0, rows, project))

    peak[...] = jnp.full_like(peak, -1e30)
    total[...] = jnp.zeros_like(total)
    acc[...] = jnp.zeros_like(acc)
    length = lens[pl.ds(roll, 1)][0, 0:1, 0:1].astype(jnp.int32)

    def attend(j):
        q_frame = me * fr_dev + lax.broadcasted_iota(jnp.int32, (block, 1), 0) // TOK_FRAME
        k_frame = j * fr_dev + lax.broadcasted_iota(jnp.int32, (1, block), 1) // TOK_FRAME
        allowed = (k_frame <= q_frame) & (k_frame < length)

        def head(h, carry):
            cols = pl.ds(pl.multiple_of(h * HEAD_DIM, HEAD_DIM), HEAD_DIM)
            q = query[:, :, cols].reshape(block, HEAD_DIM)
            k = kv[j, :, 0, :, cols].reshape(block, HEAD_DIM)
            v = kv[j, :, 1, :, cols].reshape(block, HEAD_DIM)
            scores = lax.dot_general(q, k, (((1,), (1,)), ((), ())), preferred_element_type=F32)
            scores = jnp.where(allowed, scores * scale, -1e30)
            old = peak[h]
            new = jnp.maximum(old, jnp.max(scores, axis=-1, keepdims=True))
            weights = jnp.where(allowed, jnp.exp(scores - new), 0.0)
            shrink = jnp.exp(old - new)
            peak[h] = new
            total[h] = total[h] * shrink + jnp.sum(weights, axis=-1, keepdims=True)
            acc[h] = acc[h] * shrink + jnp.dot(weights.astype(BF16), v, preferred_element_type=F32)
            return carry

        lax.fori_loop(0, heads, head, 0)

    attend(me)

    def earlier(d, carry):
        j = me - d

        @pl.when(j >= 0)
        def _():
            for s in range(T):
                pltpu.make_async_remote_copy(
                    src_ref=kv.at[j, s], dst_ref=kv.at[j, s], send_sem=kv_s.at[0, s],
                    recv_sem=kv_r.at[j, s], device_id={"seq": lax.rem(me + 1, S)},
                    device_id_type=MESH,
                ).wait_recv()
            attend(j)

        return carry

    lax.fori_loop(1, S, earlier, 0)
    for h in range(heads):
        mixed[:, h * HEAD_DIM : (h + 1) * HEAD_DIM] = (acc[h] / total[h]).astype(BF16)

    loads[1].wait()

    def out_tile(n, carry):
        cols = pl.ds(pl.multiple_of(n * tile, tile), tile)
        res = jnp.dot(mixed[...], w_out[:, cols], preferred_element_type=F32)
        part[:, :, cols] = res.astype(BF16).reshape(T, rows, tile)
        return carry

    lax.fori_loop(0, width // tile, out_tile, 0)
    after[...] = tok[...].astype(F32)
    loads[2].wait()
    loads[3].wait()

    def feed(s):
        def up_tile(n, carry):
            cols = pl.ds(pl.multiple_of(n * tile, tile), tile)
            res = jnp.dot(ag2[s], w_up[:, cols], preferred_element_type=F32)
            upbuf[:, cols] = jax.nn.gelu(res, approximate=True).astype(BF16)
            return carry

        lax.fori_loop(0, ff // tile, up_tile, 0)

        def down_tile(n, carry):
            cols = pl.ds(pl.multiple_of(n * tile, tile), tile)
            res = jnp.dot(upbuf[...], w_down[:, cols], preferred_element_type=F32)
            part[s, :, cols] = res.astype(BF16)
            return carry

        lax.fori_loop(0, width // tile, down_tile, 0)

    half = rows // 2
    hop0, finish0, drain0 = scatter(rs, 0, 0, half)
    hop1, finish1, drain1 = scatter(rs, 1, half, half)
    begin0, step0, settle0 = gather(ag2, 1, 0, half, lambda s: None)

    def renorm(first):
        span = pl.ds(first, half)
        rounded = after[span].astype(BF16).astype(F32)
        after[span] = rounded
        ag2[z, span] = rms_norm(rounded, mlp_gain[...])

    for k in range(T - 1):
        hop0(k)
    hop1(0)
    finish0()
    renorm(0)
    begin0()
    for k in range(1, T):
        if k < T - 1:
            hop1(k)
        step0(k)
    finish1()
    drain0()
    drain1()
    renorm(half)
    run_gather(*gather(ag2, 2, half, half, feed))
    settle0()
    hop2, finish2, drain2 = scatter(rs, 2, 0, rows)
    for k in range(T - 1):
        hop2(k)
    finish2()
    drain2()
    out = after[...].astype(BF16)
    hidden[...] = out
    sums = jnp.sum(out.astype(F32), axis=0, keepdims=True)
    chunks = width // LANES
    for c in range(chunks):
        fsum[z, c : c + 1, :] = sums[:, c * LANES : (c + 1) * LANES]

    def fs_send(d):
        return zcopy(fsum.at[z], fsum.at[z], fs_s.at[d], fs_r.at[z], lax.rem(z + d, T))

    for d in range(1, T):
        fs_send(d).start()
    for d in range(1, T):
        o = lax.rem(z + T - d, T)
        zcopy(fsum.at[o], fsum.at[o], fs_s.at[0], fs_r.at[o], right).wait_recv()
    per = T // fr_dev
    for f in range(fr_dev):
        m = fsum[f * per]
        for s in range(f * per + 1, (f + 1) * per):
            m = m + fsum[s]
        means[roll, me, f] = m / TOK_FRAME

    def mn_send(i, peer):
        return pltpu.make_async_remote_copy(
            src_ref=means.at[roll, me], dst_ref=means.at[roll, me], send_sem=mn_s.at[i],
            recv_sem=mn_r.at[roll, me], device_id=peer, device_id_type=MESH,
        )

    for i, peer in enumerate(peers):
        mn_send(i, peer).start()
    for a in range(DP):
        for b in range(S):
            if a or b:
                ra, sb = (lax.rem(roll + a, DP), lax.rem(me + b, S))
                pltpu.make_async_remote_copy(
                    src_ref=means.at[ra, sb], dst_ref=means.at[ra, sb], send_sem=mn_s.at[0],
                    recv_sem=mn_r.at[ra, sb], device_id=peers[0], device_id_type=MESH,
                ).wait_recv()

    lane = lax.broadcasted_iota(jnp.int32, (1, LANES), 1)
    values, gaps, valids = ([], [], [])
    for r in range(DP):
        span = lens[r]

        def frame(f, carry):
            state, vec = carry
            m = means[r, f // fr_dev, lax.rem(f, fr_dev)]
            gate = jax.nn.sigmoid(m * pool_gain[...] + pool_bias[...])
            new = gate * state + (1.0 - gate) * m
            state = jnp.where(span > f.astype(F32), new, state)
            dot = jnp.sum(jnp.sum(state * value_weight[...], axis=1, keepdims=True), axis=0, keepdims=True)
            return (state, jnp.where(lane == f, dot, vec))

        zero = (jnp.zeros((chunks, LANES), F32), jnp.zeros((1, LANES), F32))
        _, vec = lax.fori_loop(0, S * fr_dev, frame, zero)
        length_r = span[0:1].astype(jnp.int32)
        ok = lane < length_r
        vec = jnp.where(ok, vec, 0.0)
        reward = jnp.sum(jnp.where(lane == length_r - 1, vec, 0.0), axis=1, keepdims=True)
        values.append(vec)
        valids.append(ok)
        gaps.append(jnp.where(ok, reward - vec, 0.0))
    count = sum(lens[r][0:1, 0:1] for r in range(DP))
    mean = sum(jnp.sum(g, axis=1, keepdims=True) for g in gaps) / count
    centered = [jnp.where(ok, g - mean, 0.0) for ok, g in zip(valids, gaps)]
    variance = sum(jnp.sum(c * c, axis=1, keepdims=True) for c in centered) / count
    for r in range(DP):
        small[r : r + 1, :] = values[r]
        small[DP + r : DP + r + 1, :] = jnp.where(
            valids[r], centered[r] * lax.rsqrt(variance + 1e-05), 0.0
        )

    for d in range(1, T):
        fs_send(d).wait_send()
    for i, peer in enumerate(peers):
        mn_send(i, peer).wait_send()
    for d in range(1, S):

        @pl.when(me + d < S)
        def _(d=d):
            for s in range(T):
                kv_send(d, s).wait_send()


def local(
    tokens, attn_gain, w_qkv, w_out, mlp_gain, w_up, w_down, pool_gain, pool_bias, value_weight,
    valid_frames,
):
    T, S, DP = (lax.axis_size("tensor"), lax.axis_size("seq"), lax.axis_size("dp"))
    rows, width = tokens.shape[1:]
    block = rows * T
    fr_dev = block // TOK_FRAME
    chunks = width // LANES
    hcols = w_qkv.shape[2]
    heads = hcols // HEAD_DIM
    assert TOK_FRAME % rows == 0 and S * fr_dev <= LANES
    lens = jnp.broadcast_to(valid_frames.astype(F32)[:, None, None], (DP, chunks, LANES))
    vm = pl.BlockSpec(memory_space=pltpu.VMEM)
    hbm = pl.BlockSpec(memory_space=pl.ANY)
    dma = pltpu.SemaphoreType.DMA
    small_rows = -(-2 * DP // 8) * 8
    hidden, small = pl.pallas_call(
        kernel,
        out_shape=(
            jax.ShapeDtypeStruct((rows, width), BF16),
            jax.ShapeDtypeStruct((small_rows, LANES), F32),
        ),
        in_specs=[vm, vm, hbm, hbm, vm, hbm, hbm, vm, vm, vm, vm],
        out_specs=(vm, vm),
        scratch_shapes=[
            pltpu.VMEM(w_qkv.shape, BF16),
            pltpu.VMEM(w_out.shape, BF16),
            pltpu.VMEM(w_up.shape, BF16),
            pltpu.VMEM(w_down.shape, BF16),
            pltpu.VMEM((T, rows, width), BF16),
            pltpu.VMEM((T, rows, width), BF16),
            pltpu.VMEM((T, rows, hcols), BF16),
            pltpu.VMEM((S, T, 2, rows, hcols), BF16),
            pltpu.VMEM((heads, block, 1), F32),
            pltpu.VMEM((heads, block, 1), F32),
            pltpu.VMEM((heads, block, HEAD_DIM), F32),
            pltpu.VMEM((block, hcols), BF16),
            pltpu.VMEM((T, rows, width), BF16),
            pltpu.VMEM((2, T, rows, width), BF16),
            pltpu.VMEM((rows, width), F32),
            pltpu.VMEM((rows, w_up.shape[1]), BF16),
            pltpu.VMEM((T, chunks, LANES), F32),
            pltpu.VMEM((DP, S, fr_dev, chunks, LANES), F32),
            dma((4,)),
            dma((3, 2, T)),
            dma((3, T)),
            dma((S, T)),
            dma((S, T)),
            dma((3, 2, T)),
            dma((3, 2, T)),
            dma((T,)),
            dma((T,)),
            dma((DP * S,)),
            dma((DP, S)),
        ],
        compiler_params=pltpu.CompilerParams(
            collective_id=0, has_side_effects=True, vmem_limit_bytes=67043328
        ),
    )(
        tokens[0],
        attn_gain[None],
        w_qkv,
        w_out,
        mlp_gain[None],
        w_up,
        w_down,
        pool_gain.reshape(chunks, LANES),
        pool_bias.reshape(chunks, LANES),
        value_weight.reshape(chunks, LANES),
        lens,
    )
    roll, seq = (lax.axis_index("dp"), lax.axis_index("seq"))
    values = lax.dynamic_slice(small, (roll, seq * fr_dev), (1, fr_dev))
    advantages = lax.dynamic_slice(small, (DP + roll, seq * fr_dev), (1, fr_dev))
    return (hidden[None], values, advantages)


def solution(mesh):
    in_specs = (
        P("dp", ("seq", "tensor"), None),
        P(),
        P(None, None, "tensor"),
        P("tensor", None),
        P(),
        P(None, "tensor"),
        P("tensor", None),
        P(),
        P(),
        P(),
        P(),
    )
    out_specs = (P("dp", ("seq", "tensor"), None), P("dp", "seq"), P("dp", "seq"))
    return jax.shard_map(local, mesh=mesh, in_specs=in_specs, out_specs=out_specs, check_vma=False)
```
